32 devices in a mesh: farcp: 4 (over z), nearcp: 4 (over y, x), tp: 2 (over core).
Axes of the slice: x: 2, y: 2, z: 4, core: 2. Of those that a mesh axis runs over, the one named last changes fastest.
Arguments:
- raw_keys: bfloat16 [16, 8192, 8, 128], P(None, ('farcp', 'nearcp'), 'tp'), may hold values from -6 to 6
- raw_values: bfloat16 [16, 8192, 8, 128], P(None, ('farcp', 'nearcp'), 'tp'), may hold values from -6 to 6
- turn_angle: float32 [8192, 64], replicated, may hold values from -3.140625 to 3.140625
Outputs:
- stored_keys: bfloat16 [16, 8192, 8, 128], P(('farcp', 'nearcp'), None, 'tp')
- stored_values: bfloat16 [16, 8192, 8, 128], P(('farcp', 'nearcp'), None, 'tp')
- key_scale: float32 [16, 8, 128], P(('farcp', 'nearcp'), 'tp')
The draws below stay inside these ranges and needn't reach their ends.
All inputs are finite; a program needn't handle non-finite values. Where the reference program divides by a largest or mean magnitude, that divisor is 1e-20 or more.
Results may differ from the reference program's by a relative error of at most 0.001.
Values may be sent and summed in bfloat16 or wider, within the bound.
No kernel may reach another device: no remote copies, remote signals or barrier semaphores. Data moves between devices by JAX's collectives and lax.ppermute only.
A program may use at most 128 MiB of HBM per device.

```python
import jax
import jax.numpy as jnp

BATCH = 16
LENGTH = 8192
KV_HEADS = 8
HEAD_SIZE = 128
HALF_HEAD = 64


def levels(own_key, shape, cuts, low, high):
    def one(axis_at, blocks):
        steps = jax.random.uniform(jax.random.fold_in(jax.random.fold_in(own_key, 6), axis_at), (blocks,), jnp.float32, low / len(cuts), high / len(cuts))
        return jnp.repeat(jnp.exp(steps), shape[axis_at] // blocks).reshape((-1,) + (1,) * (len(shape) - axis_at - 1))

    gain = one(*cuts[0])
    for cut in cuts[1:]:
        gain = gain * one(*cut)
    return gain


def noise(stream_key, extent, scale, bound, pieces=(), kind=jnp.bfloat16):
    result = jax.random.normal(stream_key, extent, jnp.float32) * scale
    if len(pieces) > 0:
        result = levels(stream_key, extent, pieces, -0.22, 0.18) * result
    return jnp.clip(result, min=-bound, max=bound).astype(kind)


def setup_inputs(seed: int = 0) -> dict:
    arg_keys = jax.random.split(jax.random.key(seed), 4)
    return {
        "raw_keys": noise(arg_keys[0], (BATCH, LENGTH, KV_HEADS, HEAD_SIZE), 1.0, 6.0, ((1, 16), (2, 2))),
        "raw_values": noise(arg_keys[1], (BATCH, LENGTH, KV_HEADS, HEAD_SIZE), 1.0, 6.0, ((1, 16), (2, 2))),
        "turn_angle": jnp.clip(jax.random.uniform(arg_keys[2], (LENGTH, HALF_HEAD), jnp.float32, -3.140625, 3.140625), -3.140625, 3.140625),
    }


def turn_pairs(vectors, angle):
    half = vectors.shape[-1] // 2
    cosine, sine = jnp.cos(angle)[None, :, None, :], jnp.sin(angle)[None, :, None, :]
    first, second = vectors[..., :half], vectors[..., half:]
    return jnp.concatenate([first * cosine - second * sine, second * cosine + first * sine], axis=-1)


def ready_to_store(plain_keys, angle):
    wide_keys = plain_keys.astype(jnp.float32)
    return turn_pairs(wide_keys, angle)


def reference(raw_keys, raw_values, turn_angle):
    turned_keys = ready_to_store(raw_keys, turn_angle)
    key_scale = jnp.max(jnp.abs(turned_keys), axis=1)
    narrow_keys = (turned_keys / key_scale[:, None]).astype(jnp.bfloat16)
    stored_keys = narrow_keys
    stored_values = raw_values
    return stored_keys, stored_values, key_scale
```

```python
import functools

import jax
import jax.numpy as jnp
from jax import lax
from jax.experimental import pallas as pl
from jax.experimental.pallas import tpu as pltpu
from jax.sharding import PartitionSpec as P

FAR, NEAR = "farcp", "nearcp"
GROUP = (FAR, NEAR)
ANY = pl.BlockSpec(memory_space=pl.ANY)
HBM = pl.BlockSpec(memory_space=pltpu.HBM)
VMEM = pl.BlockSpec(memory_space=pltpu.VMEM)


class Plan:
    def __init__(self, mesh):
        self.far, self.near = mesh.shape[FAR], mesh.shape[NEAR]
        self.count = self.far * self.near
        self.half = self.far // 2
        shifts = sorted((f for f in range(1, self.far) if f != self.half), key=lambda f: min(f, self.far - f))
        self.early = [(f, n) for f in shifts for n in range(self.near)]
        self.early += [(0, n) for n in range(1, self.near)]
        self.late = [(self.half, n) for n in range(self.near)] if self.half else []

    def far_move(self, index, shift, back=False):
        return (index + (self.far - shift if back else shift)) % self.far

    def near_move(self, index, step, back=False):
        if self.near & (self.near - 1) == 0:
            return index ^ step
        return (index + (self.near - step if back else step)) % self.near

    def far_of(self, shift, back=False):
        index = lax.axis_index(FAR) + (self.far - shift if back else shift)
        return lax.rem(index, self.far)

    def near_of(self, step, back=False):
        return self.near_move(lax.axis_index(NEAR), step, back)

    def target(self, step):
        return self.far_of(step[0]) * self.near + self.near_of(step[1])

    def pairs(self, step):
        return [
            (f * self.near + n, self.far_move(f, step[0]) * self.near + self.near_move(n, step[1]))
            for f in range(self.far)
            for n in range(self.near)
        ]


PARAMS = pltpu.CompilerParams(vmem_limit_bytes=58 * 2**20)


def pick(plan, sources, wants, after=(), in_vmem=False):
    per = sources[0].shape[0] // plan.count
    block = (per,) + sources[0].shape[1:]
    cuts = [(w, i, s) for w, (_, srcs) in enumerate(wants) for i, s in enumerate(srcs)]
    n, m = len(sources), len(wants)

    def kernel(*refs):
        ins, refs = refs[:n], refs[n + len(after) :]
        outs, refs = refs[:m], refs[m:]
        if in_vmem:
            (arrived,) = refs
        else:
            held, arrived, left = refs
        loads, saves = [], []
        for c, (w, i, s) in enumerate(cuts):
            at = pl.multiple_of(plan.target(wants[w][0]) * per, per)
            to = outs[w].at[i] if in_vmem else held.at[c]
            loads.append(pltpu.make_async_copy(ins[s].at[pl.ds(at, per)], to, arrived.at[c]))
            loads[-1].start()
        for c, (w, i, s) in enumerate(cuts):
            loads[c].wait()
            if not in_vmem:
                saves.append(pltpu.make_async_copy(held.at[c], outs[w].at[i], left.at[c]))
                saves[-1].start()
        for save in saves:
            save.wait()

    dtype = sources[0].dtype
    sems = [pltpu.SemaphoreType.DMA((len(cuts),))]
    scratch = sems if in_vmem else [pltpu.VMEM((len(cuts),) + block, dtype)] + sems * 2
    return pl.pallas_call(
        kernel,
        out_shape=[jax.ShapeDtypeStruct((len(srcs),) + block, dtype) for _, srcs in wants],
        in_specs=[HBM] * n + [ANY] * len(after),
        out_specs=[VMEM if in_vmem else HBM] * m,
        scratch_shapes=scratch,
        compiler_params=PARAMS,
    )(*sources, *after)


def own(plan, source, step, part):
    per = source.shape[0] // plan.count
    rows, lanes = source.shape[1:]
    blocks = plan.near if part else plan.count

    def kernel(src, out, held, sem):
        me = plan.target(step)
        load = pltpu.make_async_copy(src.at[pl.ds(pl.multiple_of(me * per, per), per)], held, sem)
        load.start()
        load.wait()
        at = (plan.near_of(0) if part else me) * rows
        save = pltpu.make_async_copy(held, out.at[:, pl.ds(pl.multiple_of(at, rows), rows)], sem)
        save.start()
        save.wait()

    return pl.pallas_call(
        kernel,
        out_shape=jax.ShapeDtypeStruct((per, rows * blocks, lanes), source.dtype),
        in_specs=[HBM],
        out_specs=HBM,
        scratch_shapes=[pltpu.VMEM((per, rows, lanes), source.dtype), pltpu.SemaphoreType.DMA],
        compiler_params=PARAMS,
    )(source)


def put(plan, targets, block, step):
    _, per, rows, lanes = block.shape
    old = [i for i, target in enumerate(targets) if not isinstance(target, jax.ShapeDtypeStruct)]
    n, m = len(targets), len(old)

    def kernel(*refs):
        got, outs, sems = refs[m], refs[m + 1 : m + n + 1], refs[m + n + 1]
        saves = []
        for i, out in enumerate(outs):
            at = plan.near_of(step[1], back=True)
            if out.shape[1] == rows * plan.count:
                at = plan.far_of(step[0], back=True) * plan.near + at
            to = out.at[:, pl.ds(pl.multiple_of(at * rows, rows), rows)]
            saves.append(pltpu.make_async_copy(got.at[i], to, sems.at[i]))
            saves[-1].start()
        for save in saves:
            save.wait()

    return pl.pallas_call(
        kernel,
        out_shape=[jax.ShapeDtypeStruct(t.shape, t.dtype) for t in targets],
        in_specs=[HBM] * m + [VMEM],
        out_specs=[HBM] * n,
        scratch_shapes=[pltpu.SemaphoreType.DMA((n,))],
        input_output_aliases={j: i for j, i in enumerate(old)},
        compiler_params=PARAMS,
    )(*[targets[i] for i in old], block)


def turn_pairs(vectors, angle):
    half = vectors.shape[-1] // 2
    cosine, sine = (jnp.cos(angle)[None, :, None, :], jnp.sin(angle)[None, :, None, :])
    first, second = (vectors[..., :half], vectors[..., half:])
    return jnp.concatenate(
        [first * cosine - second * sine, second * cosine + first * sine], axis=-1
    )


def body(plan, raw_keys, raw_values, turn_angle):
    batch, length, heads, size = raw_keys.shape
    per, rows = batch // plan.count, length * heads
    flat = [raw_keys.reshape(batch, rows, size), raw_values.reshape(batch, rows, size)]
    part_length = length * plan.near
    part = jax.ShapeDtypeStruct((per, rows * plan.near, size), raw_keys.dtype)

    def send(block, step):
        return lax.ppermute(block, GROUP, plan.pairs(step))

    both, one = (0, 1), (0,)
    head = pick(plan, flat, [(step, both) for step in plan.early[:1]], in_vmem=True)
    got_early = [send(b, step) for b, step in zip(head, plan.early)]
    wants = [(step, both) for step in plan.early[1:]] + [(step, one) for step in plan.late]
    blocks = pick(plan, flat, wants, after=head)
    got_early += [send(b, step) for b, step in zip(blocks, plan.early[1:])]
    got_keys = [send(b, step) for b, step in zip(blocks[len(plan.early) - 1 :], plan.late)]
    blocks = pick(plan, flat[1:], [(step, one) for step in plan.late], after=blocks[:1])
    got_values = [send(b, step) for b, step in zip(blocks, plan.late)]

    parts = {0: own(plan, flat[0], (0, 0), True)}
    values = own(plan, flat[1], (0, 0), False)
    for block, step in zip(got_early, plan.early):
        parts[step[0]], values = put(plan, [parts.get(step[0], part), values], block, step)

    def turned_part(shift):
        start = plan.far_of(shift, back=True) * part_length
        angle = lax.dynamic_slice_in_dim(turn_angle, start, part_length, 0)
        plain = parts[shift].reshape(per, part_length, heads, size)
        turned = turn_pairs(plain.astype(jnp.float32), angle)
        return turned, jnp.max(jnp.abs(turned), axis=1)

    turned = {shift: turned_part(shift) for shift in parts}
    if plan.late:
        turned, got_keys[0] = lax.optimization_barrier((turned, got_keys[0]))
        parts[plan.half] = part
        for block, step in zip(got_keys, plan.late):
            (parts[plan.half],) = put(plan, [parts[plan.half]], block, step)
        turned[plan.half] = turned_part(plan.half)
    key_scale = functools.reduce(jnp.maximum, [most for _, most in turned.values()])
    narrow_keys = jnp.zeros((per, part_length * plan.far, heads, size), jnp.bfloat16)
    for shift, (vectors, _) in turned.items():
        narrow = (vectors / key_scale[:, None]).astype(jnp.bfloat16)
        start = plan.far_of(shift, back=True) * part_length
        narrow_keys = lax.dynamic_update_slice_in_dim(narrow_keys, narrow, start, 1)
    narrow_keys, key_scale, values = lax.optimization_barrier((narrow_keys, key_scale, values))
    for block, step in zip(got_values, plan.late):
        (values,) = put(plan, [values], block, step)
    stored_values = values.reshape(per, part_length * plan.far, heads, size)
    return (narrow_keys, stored_values, key_scale)


def solution(mesh):
    placed = (
        P(None, GROUP, "tp", None),
        P(None, GROUP, "tp", None),
        P(),
    )
    return jax.shard_map(
        functools.partial(body, Plan(mesh)),
        mesh=mesh,
        in_specs=placed,
        out_specs=(
            P(GROUP, None, "tp", None),
            P(GROUP, None, "tp", None),
            P(GROUP, "tp", None),
        ),
        check_vma=False,
    )
```
